32 devices in a mesh: dp: 32 (over z, y, x, core), rank: 1.
Axes of the slice: x: 2, y: 2, z: 4, core: 2. Of those that a mesh axis runs over, the one named last changes fastest.
Arguments:
- cloud_x: float32 [64, 65536], P(None, 'dp'), may hold values from -0.6 to 0.6
- cloud_y: float32 [64, 65536], P(None, 'dp'), may hold values from -0.6 to 0.6
- mass_x: float32 [65536], P('dp'), may hold values from 0.25 to 4
- mass_y: float32 [65536], P('dp'), may hold values from 0.25 to 4
- left_start: float32 [256, 65536], P('rank', 'dp'), may hold values from 0.25 to 204.8
- right_start: float32 [256, 65536], P('rank', 'dp'), may hold values from 0.25 to 204.8
- weight_start: float32 [256], P('rank'), may hold values from 0.25 to 4
Outputs:
- left_factor: float32 [256, 65536], P('rank', 'dp')
- right_factor: float32 [256, 65536], P('rank', 'dp')
- rank_weights: float32 [256], P('rank')
The draws below stay inside these ranges and needn't reach their ends.
All inputs are finite; a program needn't handle non-finite values.
Results may differ from the reference program's by a relative error of at most 0.0003.
Values sent between devices are 32-bit elements; how exact they have to be, the bound alone decides.
A program may use at most 64 MiB of HBM per device.

```python
import math
import jax
import jax.numpy as jnp
from jax import lax

DIM = 64
RANK = 256
INNER = 4
MIRROR = 3
N = 65536


def cluster_layout(key):
    centres = jax.random.normal(jax.random.fold_in(key, 7101), (DIM, RANK), jnp.float32) * jnp.sqrt(0.6 / DIM)
    shifted = centres + jax.random.normal(jax.random.fold_in(key, 7102), (DIM, RANK), jnp.float32) * jnp.sqrt(0.2 / DIM)
    member_x = jax.random.randint(jax.random.fold_in(key, 7103), (N,), 0, RANK).astype(jnp.int32)
    member_y = jax.random.randint(jax.random.fold_in(key, 7104), (N,), 0, RANK).astype(jnp.int32)
    return (centres, shifted, member_x, member_y)


def cloud_points(key, centres, member, salt):
    base = jnp.take(centres, member, axis=1)
    noise_key = jax.random.fold_in(key, salt)
    noise = jax.random.normal(noise_key, (DIM, N), jnp.float32) * jnp.sqrt(0.5 / DIM)
    return jnp.clip(base + noise, -0.6, 0.6)


def factor_start(key, member, salt):
    rest = jnp.exp(jax.random.uniform(jax.random.fold_in(key, salt), (RANK, N), jnp.float32, jnp.log(0.25), jnp.log(4.0)))
    own = RANK * jnp.exp(jax.random.uniform(jax.random.fold_in(key, salt + 1), (RANK, N), jnp.float32, jnp.log(0.25), jnp.log(0.8)))
    match = jnp.arange(RANK, dtype=jnp.int32)[:, None] == member[None, :]
    return jnp.where(match, own, rest)


def draw_cloud_x(key, part):
    centres, shifted, member_x, member_y = cluster_layout(key)
    return cloud_points(key, centres, member_x, 7201)


def draw_cloud_y(key, part):
    centres, shifted, member_x, member_y = cluster_layout(key)
    return cloud_points(key, shifted, member_y, 7301)


def draw_left_start(key, part):
    centres, shifted, member_x, member_y = cluster_layout(key)
    return factor_start(key, member_x, 7401)


def draw_right_start(key, part):
    centres, shifted, member_x, member_y = cluster_layout(key)
    return factor_start(key, member_y, 7501)


def level_of(key, extent, shards, least, largest):
    def one(dim, shards_of):
        steps = jax.random.uniform(jax.random.fold_in(jax.random.fold_in(key, 6), dim), (shards_of,), jnp.float32, least / len(shards), largest / len(shards))
        return jnp.repeat(jnp.exp(steps), extent[dim] // shards_of).reshape((-1,) + (1,) * (len(extent) - dim - 1))

    gain = one(*shards[0])
    for cut in shards[1:]:
        gain = gain * one(*cut)
    return gain


def setup_inputs(seed: int = 0) -> dict:
    key_of = jax.random.split(jax.random.key(seed), 8)
    cloud_x = draw_cloud_x(jax.random.fold_in(key_of[7], 71), 0)
    cloud_y = draw_cloud_y(jax.random.fold_in(key_of[7], 71), 0)
    mass_x = jnp.clip(jnp.exp(math.log(4.0) - 2.7725887 * jax.random.uniform(key_of[2], (N,), jnp.float32) ** level_of(key_of[2], (N,), ((0, 32),), -0.2, 0.2)), 0.25, 4.0)
    mass_y = jnp.clip(jnp.exp(math.log(4.0) - 2.7725887 * jax.random.uniform(key_of[3], (N,), jnp.float32) ** level_of(key_of[3], (N,), ((0, 32),), -0.2, 0.2)), 0.25, 4.0)
    left_start = draw_left_start(jax.random.fold_in(key_of[7], 71), 0)
    right_start = draw_right_start(jax.random.fold_in(key_of[7], 71), 0)
    weight_start = jnp.clip(jnp.exp(jax.random.uniform(key_of[6], (RANK,), jnp.float32, math.log(0.25), math.log(4.0))), 0.25, 4.0)
    return dict(cloud_x=cloud_x, cloud_y=cloud_y, mass_x=mass_x, mass_y=mass_y, left_start=left_start, right_start=right_start, weight_start=weight_start)


exact_mode = lax.Precision.HIGHEST
step_size = 2.0


def project(kernel_left, kernel_right, kernel_weight, left_mass, right_mass):
    scale_left = jnp.ones((RANK,), jnp.float32)
    scale_right = jnp.ones((RANK,), jnp.float32)
    for repeat in range(INNER):
        point_left = left_mass / jnp.dot(scale_left, kernel_left, precision=exact_mode)
        point_right = right_mass / jnp.dot(scale_right, kernel_right, precision=exact_mode)
        column_left = jnp.dot(kernel_left, point_left, precision=exact_mode)
        column_right = jnp.dot(kernel_right, point_right, precision=exact_mode)
        weights = jnp.cbrt(kernel_weight * scale_left * column_left * scale_right * column_right)
        scale_left = weights / column_left
        scale_right = weights / column_right
    left = point_left[None, :] * kernel_left * scale_left[:, None]
    right = point_right[None, :] * kernel_right * scale_right[:, None]
    return left, right, weights


def moments(cloud, factor):
    product = jnp.dot(cloud, factor.T, precision=exact_mode)
    square = jnp.dot(factor, jnp.sum(cloud * cloud, axis=0), precision=exact_mode)
    column = jnp.sum(factor, axis=1)
    return product, square, column


def reference(cloud_x, cloud_y, mass_x, mass_y, left_start, right_start, weight_start):
    left_mass = mass_x * (N / jnp.sum(mass_x))
    right_mass = mass_y * (N / jnp.sum(mass_y))
    left, right, weights = project(left_start, right_start, weight_start, left_mass, right_mass)
    for outer in range(MIRROR):
        prod_x, square_x, sums_q = moments(cloud_x, left)
        prod_y, square_y, sums_r = moments(cloud_y, right)
        grad_q = square_y / weights
        grad_r = square_x / weights
        grad_g = -(square_x * sums_r + sums_q * square_y - 2.0 * jnp.sum(prod_x * prod_y, axis=0)) / (weights * weights)
        mean_q = jnp.sum(grad_q) / RANK
        mean_r = jnp.sum(grad_r) / RANK
        mean_g = jnp.sum(grad_g) / RANK
        field_q = (grad_q - mean_q)[:, None] - 2.0 * jnp.dot(prod_y.T, cloud_x, precision=exact_mode) / weights[:, None]
        field_r = (grad_r - mean_r)[:, None] - 2.0 * jnp.dot(prod_x.T, cloud_y, precision=exact_mode) / weights[:, None]
        kernel_left = left * jnp.exp(-step_size * field_q)
        kernel_right = right * jnp.exp(-step_size * field_r)
        kernel_weight = weights * jnp.exp(-step_size * (grad_g - mean_g))
        left, right, weights = project(kernel_left, kernel_right, kernel_weight, left_mass, right_mass)
    return RANK * left, RANK * right, (RANK / N) * weights
```

```python
import functools
import math

import jax
import jax.numpy as jnp
from jax import lax
from jax.experimental import pallas as pl
from jax.experimental.pallas import tpu as pltpu
from jax.sharding import PartitionSpec as P

RANK = 256
INNER = 4
MIRROR = 3


exact_mode = lax.Precision.HIGHEST
step_size = 2.0


def moments(cloud, factor):
    product = jnp.dot(cloud, factor.T, precision=exact_mode)
    square = jnp.dot(factor, jnp.sum(cloud * cloud, axis=0), precision=exact_mode)
    column = jnp.sum(factor, axis=1)
    return (product, square, column)


def widen(local_part, offset):
    shape_full = local_part.shape[:-1] + (RANK,)
    starts = (0,) * (local_part.ndim - 1) + (offset,)
    return lax.dynamic_update_slice(jnp.zeros(shape_full, jnp.float32), local_part, starts)


def narrow(full_part, offset, ranks_local):
    return lax.dynamic_slice_in_dim(full_part, offset, ranks_local, full_part.ndim - 1)


def shards(cloud_x, cloud_y, mass_x, mass_y, left_start, right_start, weight_start):
    ranks_local = left_start.shape[0]
    points_dev = left_start.shape[1]
    total_count = float(points_dev * lax.axis_size("dp"))
    offset = lax.axis_index("rank") * ranks_local
    mass_sums = lax.psum((jnp.sum(mass_x), jnp.sum(mass_y)), "dp")
    left_mass = mass_x * (total_count / mass_sums[0])
    right_mass = mass_y * (total_count / mass_sums[1])

    def project(kernel_left, kernel_right, kernel_weight):
        scale_left = jnp.ones((ranks_local,), jnp.float32)
        scale_right = jnp.ones((ranks_local,), jnp.float32)
        for repeat in range(INNER):
            row_left, row_right = lax.psum(
                (
                    jnp.dot(scale_left, kernel_left, precision=exact_mode),
                    jnp.dot(scale_right, kernel_right, precision=exact_mode),
                ),
                "rank",
            )
            point_left = left_mass / row_left
            point_right = right_mass / row_right
            column_left, column_right = lax.psum(
                (
                    jnp.dot(kernel_left, point_left, precision=exact_mode),
                    jnp.dot(kernel_right, point_right, precision=exact_mode),
                ),
                "dp",
            )
            weights = jnp.cbrt(
                kernel_weight * scale_left * column_left * scale_right * column_right
            )
            scale_left = weights / column_left
            scale_right = weights / column_right
        left = point_left[None, :] * kernel_left * scale_left[:, None]
        right = point_right[None, :] * kernel_right * scale_right[:, None]
        return (left, right, weights)

    left, right, weights = project(left_start, right_start, weight_start)
    for outer in range(MIRROR):
        prod_x, square_x, sums_q = moments(cloud_x, left)
        prod_y, square_y, sums_r = moments(cloud_y, right)
        root_weights = jnp.where(lax.axis_index("dp") == 0, weights, jnp.zeros_like(weights))
        full_px, full_py, full_sx, full_sy, full_q, full_r, full_w = lax.psum(
            (
                widen(prod_x, offset),
                widen(prod_y, offset),
                widen(square_x, offset),
                widen(square_y, offset),
                widen(sums_q, offset),
                widen(sums_r, offset),
                widen(root_weights, offset),
            ),
            ("dp", "rank"),
        )
        full_gq = full_sy / full_w
        full_gr = full_sx / full_w
        full_gg = -(
            full_sx * full_r + full_q * full_sy - 2.0 * jnp.sum(full_px * full_py, axis=0)
        ) / (full_w * full_w)
        mean_q = jnp.sum(full_gq) / RANK
        mean_r = jnp.sum(full_gr) / RANK
        mean_g = jnp.sum(full_gg) / RANK
        prod_x = narrow(full_px, offset, ranks_local)
        prod_y = narrow(full_py, offset, ranks_local)
        grad_q = narrow(full_gq, offset, ranks_local)
        grad_r = narrow(full_gr, offset, ranks_local)
        grad_g = narrow(full_gg, offset, ranks_local)
        field_q = (grad_q - mean_q)[:, None] - 2.0 * jnp.dot(
            prod_y.T, cloud_x, precision=exact_mode
        ) / weights[:, None]
        field_r = (grad_r - mean_r)[:, None] - 2.0 * jnp.dot(
            prod_x.T, cloud_y, precision=exact_mode
        ) / weights[:, None]
        kernel_left = left * jnp.exp(-step_size * field_q)
        kernel_right = right * jnp.exp(-step_size * field_r)
        kernel_weight = weights * jnp.exp(-step_size * (grad_g - mean_g))
        left, right, weights = project(kernel_left, kernel_right, kernel_weight)
    return (RANK * left, RANK * right, weights * (RANK / total_count))


PLANE = 8
LANE = 128
AUG = 80
LOG2E = math.log2(math.e)
MESH = pl.DeviceIdType.MESH


def split(x):
    high = x.astype(jnp.bfloat16)
    low = (x - high.astype(jnp.float32)).astype(jnp.bfloat16)
    return high, low


def cube_root(x):
    y = jnp.exp(jnp.log(x) * (1.0 / 3.0))
    y = y - (y - x / (y * y)) * (1.0 / 3.0)
    return jnp.where(x > 0.0, y, x)


def fused_kernel(
    devices,
    cx_ref, cy_ref, mx_ref, my_ref, ls_ref, rs_ref, ws_ref,
    lo_ref, ro_ref, wo_ref,
    kl, kr, vl, vr, ul, ur, pl_ref, pr_ref,
    xh, xl, yh, yl, mom, weight_ref, sl_ref, sr_ref, coef_h, coef_l,
    pay, got1, pay2, got2,
    bpay, bgot1, bpay2, bgot2,
    cgot1, cpay2, cgot2, full,
    s_sem1, r_sem1, s_sem2, r_sem2, s_sem3, r_sem3, bs_sem1, br_sem1, bs_sem2, br_sem2,
    cs_sem1, cr_sem1, cs_sem2, cr_sem2,
):
    ranks, points = ls_ref.shape
    dims = cx_ref.shape[0]
    total_count = float(points * devices)
    planes = devices // PLANE
    halves = ranks // LANE
    tiles = points // LANE
    blocks = ranks // 8
    me = lax.axis_index("dp")
    spot = lax.rem(me, PLANE)
    level = lax.div(me, PLANE)

    def in_plane(shift):
        return level * PLANE + lax.rem(spot + shift, PLANE)

    def across(shift):
        return lax.rem(level + shift, planes) * PLANE + spot

    barrier = pltpu.get_barrier_semaphore()
    for shift in range(1, PLANE):
        pl.semaphore_signal(barrier, inc=1, device_id={"dp": in_plane(shift)}, device_id_type=MESH)
    for shift in range(1, planes):
        pl.semaphore_signal(barrier, inc=1, device_id={"dp": across(shift)}, device_id_type=MESH)

    def send(src, dst, s_sem, r_sem, target):
        copy = pltpu.make_async_remote_copy(
            src_ref=src, dst_ref=dst, send_sem=s_sem, recv_sem=r_sem,
            device_id={"dp": target}, device_id_type=MESH,
        )
        copy.start()
        return copy

    def scatter_plane(src, got, s_sems, r_sems):
        return [
            send(src, got.at[spot], s_sems.at[shift], r_sems.at[shift], in_plane(shift))
            for shift in range(1, PLANE)
        ]

    def scatter_across(src, got, s_sems, r_sems):
        return [
            send(src, got.at[level], s_sems.at[shift], r_sems.at[shift], across(shift))
            for shift in range(1, planes)
        ]

    def finish(copies):
        for copy in copies:
            copy.wait_recv()
        for copy in copies:
            copy.wait_send()

    def total_of(got, count):
        acc = got[0]
        for i in range(1, count):
            acc = acc + got[i]
        return acc

    def reduce_all(value, parity, p1, g1, p2, g2, ss1, rs1, ss2, rs2):
        src = p1.at[parity]
        src[...] = value
        g1.at[parity][spot] = value
        finish(scatter_plane(src, g1.at[parity], ss1.at[parity], rs1.at[parity]))
        part = total_of(g1.at[parity], PLANE)
        src2 = p2.at[parity]
        src2[...] = part
        g2.at[parity][level] = part
        finish(scatter_across(src2, g2.at[parity], ss2.at[parity], rs2.at[parity]))
        return total_of(g2.at[parity], planes)

    def small_reduce(value, parity):
        return reduce_all(value, parity, pay, got1, pay2, got2, s_sem1, r_sem1, s_sem2, r_sem2)

    def spread(dst, value):
        for h in range(halves):
            square = jnp.broadcast_to(value[h : h + 1, :], (LANE, LANE))
            dst[h * LANE : (h + 1) * LANE, :] = square.T

    def row_of(b):
        return pl.ds(pl.multiple_of(b * 8, 8), 8)

    def rows_pass():
        def body(b, acc):
            al, ar = acc
            rows = row_of(b)
            al = al + kl[rows, :] * jnp.concatenate([vl[rows, :]] * tiles, axis=1)
            ar = ar + kr[rows, :] * jnp.concatenate([vr[rows, :]] * tiles, axis=1)
            return al, ar

        zero = jnp.zeros((8, points), jnp.float32)
        al, ar = lax.fori_loop(0, blocks, body, (zero, zero), unroll=4)
        ul[...] = jnp.broadcast_to(sl_ref[...] / jnp.sum(al, axis=0, keepdims=True), (8, points))
        ur[...] = jnp.broadcast_to(sr_ref[...] / jnp.sum(ar, axis=0, keepdims=True), (8, points))

    def columns_pass():
        bl, br = ul[...], ur[...]

        def fold(x):
            parts = [x[:, i * LANE : (i + 1) * LANE] for i in range(tiles)]
            while len(parts) > 1:
                parts = [parts[i] + parts[i + 1] for i in range(0, len(parts) - 1, 2)] + (
                    parts[-1:] if len(parts) % 2 else []
                )
            return parts[0]

        def body(b, carry):
            rows = row_of(b)
            pl_ref[rows, :] = fold(kl[rows, :] * bl)
            pr_ref[rows, :] = fold(kr[rows, :] * br)
            return carry

        lax.fori_loop(0, blocks, body, 0, unroll=4)
        out = []
        for ref in (pl_ref, pr_ref):
            for h in range(halves):
                out.append(jnp.sum(ref[h * LANE : (h + 1) * LANE, :].T, axis=0, keepdims=True))
        return jnp.concatenate(out, axis=0)

    def rescale(cl, cr, v1, v2):
        g = cube_root(weight_ref[...] * v1 * cl * v2 * cr)
        v1, v2 = g / cl, g / cr
        spread(vl, v1)
        spread(vr, v2)
        return g, v1, v2

    def small_step(parity, v1, v2):
        rows_pass()
        sums = small_reduce(columns_pass(), parity)
        return rescale(sums[:halves], sums[halves : 2 * halves], v1, v2)

    for src, high, low in ((cx_ref, xh, xl), (cy_ref, yh, yl)):
        cloud = src[...]
        square = jnp.sum(cloud * cloud, axis=0, keepdims=True)
        place = lax.broadcasted_iota(jnp.int32, (LANE - dims, points), 0)
        extra = jnp.where(place == 0, square, jnp.where(place == 1, 1.0, 0.0))
        high[:dims, :], low[:dims, :] = split(cloud)
        high[dims:, :], low[dims:, :] = split(extra)
    ones = jnp.ones((halves, LANE), jnp.float32)
    weight_ref[...] = ws_ref[...]
    vl[...] = jnp.ones((ranks, LANE), jnp.float32)
    vr[...] = jnp.ones((ranks, LANE), jnp.float32)
    sl_ref[...] = mx_ref[...]
    sr_ref[...] = my_ref[...]
    kl[...] = ls_ref[...]
    kr[...] = rs_ref[...]
    rows_pass()
    first = columns_pass()
    pl.semaphore_wait(barrier, PLANE - 1 + planes - 1)

    sums = small_reduce(first, 0)
    cl, cr = sums[:halves], sums[halves : 2 * halves]
    al = total_count / jnp.sum(cl)
    ar = total_count / jnp.sum(cr)
    sl_ref[...] = sl_ref[...] * al
    sr_ref[...] = sr_ref[...] * ar
    g, v1, v2 = rescale(cl * al, cr * ar, ones, ones)

    def inner(i, carry):
        _, v1, v2 = carry
        return small_step(lax.rem(i, 2), v1, v2)

    _, v1, v2 = lax.fori_loop(1, INNER - 1, inner, (g, v1, v2))

    chunk = 2 * LANE

    def moment_pass(k_ref, u_ref, high, low):
        acc = jnp.zeros((AUG, ranks), jnp.float32)
        nt = (((1,), (1,)), ((), ()))
        for c in range(points // chunk):
            cols = slice(c * chunk, (c + 1) * chunk)
            w = k_ref[:, cols] * u_ref[0:1, cols]
            wh, wl = split(w)
            h, l = high[:AUG, cols], low[:AUG, cols]
            acc = acc + lax.dot_general(h, wh, nt, preferred_element_type=jnp.float32)
            acc = acc + lax.dot_general(h, wl, nt, preferred_element_type=jnp.float32)
            acc = acc + lax.dot_general(l, wh, nt, preferred_element_type=jnp.float32)
        return acc

    def lanes(row):
        return [row[:, h * LANE : (h + 1) * LANE] for h in range(halves)]

    def wide(value):
        return jnp.concatenate([value[h : h + 1, :] for h in range(halves)], axis=1)

    def update(k_ref, u_ref, v_ref, high, low):
        for c in range(points // chunk):
            cols = slice(c * chunk, (c + 1) * chunk)
            h, l = high[:, cols], low[:, cols]
            a, b = coef_h[...], coef_l[...]
            e = jnp.dot(a, h, preferred_element_type=jnp.float32)
            e = e + jnp.dot(a, l, preferred_element_type=jnp.float32)
            e = e + jnp.dot(b, h, preferred_element_type=jnp.float32)
            scale = jnp.concatenate([v_ref[...]] * (chunk // LANE), axis=1)
            k_ref[:, cols] = k_ref[:, cols] * u_ref[0:1, cols] * scale * jnp.exp2(e)

    per = dims // PLANE

    def coefficients(centre, moment):
        mean = jnp.sum(moment) / ranks
        bias = (-2.0 * LOG2E) * (moment - mean)
        place = lax.broadcasted_iota(jnp.int32, (LANE - dims, ranks), 0)
        extra = jnp.where(place == 1, bias, 0.0)
        full_rows = jnp.concatenate([centre * (4.0 * LOG2E), extra], axis=0)
        high, low = split(full_rows.T)
        coef_h[...] = high
        coef_l[...] = low

    def outer_step(outer, carry):
        v1, v2 = carry
        rows_pass()
        mom_x = moment_pass(kl, ul, xh, xl)
        mom_y = moment_pass(kr, ur, yh, yl)
        for j in range(PLANE):
            mom[j, 0] = mom_x[j * per : (j + 1) * per]
            mom[j, 1] = mom_y[j * per : (j + 1) * per]
        copies = []
        for shift in range(1, PLANE):
            target = lax.rem(spot + shift, PLANE)
            copies.append(
                send(mom.at[target], cgot1.at[spot], cs_sem1.at[shift], cr_sem1.at[shift], in_plane(shift))
            )
        cgot1[spot] = mom[spot]
        value = jnp.concatenate(
            lanes(mom_x[dims + 1 : dims + 2]) + lanes(mom_y[dims + 1 : dims + 2])
            + lanes(mom_x[dims : dims + 1]) + lanes(mom_y[dims : dims + 1]),
            axis=0,
        )
        bpay[...] = value
        bgot1[spot] = value
        small = scatter_plane(bpay, bgot1, bs_sem1, br_sem1)
        finish(small)
        part = total_of(bgot1, PLANE)
        bpay2[...] = part
        bgot2[level] = part
        small = scatter_across(bpay2, bgot2, bs_sem2, br_sem2)
        finish(copies)
        part = total_of(cgot1, PLANE)
        cpay2[...] = part
        cgot2[level] = part
        copies = scatter_across(cpay2, cgot2, cs_sem2, cr_sem2)
        finish(small)
        sums = total_of(bgot2, planes)
        cl, cr = sums[:halves], sums[halves : 2 * halves]
        sx = wide(sums[2 * halves : 3 * halves] / cl)
        sy = wide(sums[3 * halves : 4 * halves] / cr)
        g, v1, v2 = rescale(cl, cr, v1, v2)
        finish(copies)
        full[spot] = total_of(cgot2, planes)
        finish(
            [
                send(full.at[spot], full.at[spot], s_sem3.at[shift], r_sem3.at[shift], in_plane(shift))
                for shift in range(1, PLANE)
            ]
        )
        inv_l, inv_r = wide(1.0 / cl), wide(1.0 / cr)
        centre_x = jnp.concatenate([full[j, 0] for j in range(PLANE)], axis=0) * inv_l
        centre_y = jnp.concatenate([full[j, 1] for j in range(PLANE)], axis=0) * inv_r
        coefficients(centre_y, sy)
        update(kl, ul, vl, xh, xl)
        coefficients(centre_x, sx)
        update(kr, ur, vr, yh, yl)
        gg = -(sx + sy - 2.0 * jnp.sum(centre_x * centre_y, axis=0, keepdims=True))
        tilt = jnp.exp(-step_size * (gg - jnp.sum(gg) / ranks))
        weight_ref[...] = g * jnp.concatenate(lanes(tilt), axis=0)
        vl[...] = jnp.ones((ranks, LANE), jnp.float32)
        vr[...] = jnp.ones((ranks, LANE), jnp.float32)
        carry = (g, ones, ones)
        steps = jnp.where(outer == MIRROR - 1, INNER, INNER - 1)

        def again(i, carry):
            return small_step(lax.rem(i + 1, 2), carry[1], carry[2])

        g, v1, v2 = lax.fori_loop(0, steps, again, carry)
        wo_ref[...] = g * (ranks / total_count)
        return v1, v2

    lax.fori_loop(0, MIRROR, outer_step, (v1, v2))

    def emit(b, carry):
        rows = row_of(b)
        sl = jnp.concatenate([vl[rows, :]] * tiles, axis=1)
        sr = jnp.concatenate([vr[rows, :]] * tiles, axis=1)
        lo_ref[rows, :] = kl[rows, :] * ul[...] * sl * float(ranks)
        ro_ref[rows, :] = kr[rows, :] * ur[...] * sr * float(ranks)
        return carry

    lax.fori_loop(0, blocks, emit, 0)


def fused(cloud_x, cloud_y, mass_x, mass_y, left_start, right_start, weight_start):
    devices = lax.axis_size("dp")
    ranks, points = left_start.shape
    dims = cloud_x.shape[0]
    planes = devices // PLANE
    halves = ranks // LANE
    per = dims // PLANE
    f32 = jnp.float32
    dma = pltpu.SemaphoreType.DMA
    vmem = pl.BlockSpec(memory_space=pltpu.VMEM)
    left, right, weights = pl.pallas_call(
        functools.partial(fused_kernel, devices),
        out_shape=(
            jax.ShapeDtypeStruct((ranks, points), f32),
            jax.ShapeDtypeStruct((ranks, points), f32),
            jax.ShapeDtypeStruct((halves, LANE), f32),
        ),
        in_specs=[vmem] * 7,
        out_specs=(vmem,) * 3,
        scratch_shapes=[
            pltpu.VMEM((ranks, points), f32),
            pltpu.VMEM((ranks, points), f32),
            pltpu.VMEM((ranks, LANE), f32),
            pltpu.VMEM((ranks, LANE), f32),
            pltpu.VMEM((8, points), f32),
            pltpu.VMEM((8, points), f32),
            pltpu.VMEM((ranks, LANE), f32),
            pltpu.VMEM((ranks, LANE), f32),
            pltpu.VMEM((LANE, points), jnp.bfloat16),
            pltpu.VMEM((LANE, points), jnp.bfloat16),
            pltpu.VMEM((LANE, points), jnp.bfloat16),
            pltpu.VMEM((LANE, points), jnp.bfloat16),
            pltpu.VMEM((PLANE, 2, per, ranks), f32),
            pltpu.VMEM((halves, LANE), f32),
            pltpu.VMEM((1, points), f32),
            pltpu.VMEM((1, points), f32),
            pltpu.VMEM((ranks, LANE), jnp.bfloat16),
            pltpu.VMEM((ranks, LANE), jnp.bfloat16),
            pltpu.VMEM((2, 2 * halves, LANE), f32),
            pltpu.VMEM((2, PLANE, 2 * halves, LANE), f32),
            pltpu.VMEM((2, 2 * halves, LANE), f32),
            pltpu.VMEM((2, planes, 2 * halves, LANE), f32),
            pltpu.VMEM((4 * halves, LANE), f32),
            pltpu.VMEM((PLANE, 4 * halves, LANE), f32),
            pltpu.VMEM((4 * halves, LANE), f32),
            pltpu.VMEM((planes, 4 * halves, LANE), f32),
            pltpu.VMEM((PLANE, 2, per, ranks), f32),
            pltpu.VMEM((2, per, ranks), f32),
            pltpu.VMEM((planes, 2, per, ranks), f32),
            pltpu.VMEM((PLANE, 2, per, ranks), f32),
            dma((2, PLANE)), dma((2, PLANE)), dma((2, planes)), dma((2, planes)),
            dma((PLANE,)), dma((PLANE,)),
            dma((PLANE,)), dma((PLANE,)), dma((planes,)), dma((planes,)),
            dma((PLANE,)), dma((PLANE,)), dma((planes,)), dma((planes,)),
        ],
        compiler_params=pltpu.CompilerParams(
            collective_id=0, has_side_effects=True, vmem_limit_bytes=48 * 1024 * 1024
        ),
        name="sinkhorn",
    )(
        cloud_x, cloud_y, mass_x.reshape(1, points), mass_y.reshape(1, points),
        left_start, right_start, weight_start.reshape(halves, LANE),
    )
    return left, right, weights.reshape(ranks)


def solution(mesh):
    in_specs = (
        P(None, "dp"),
        P(None, "dp"),
        P("dp"),
        P("dp"),
        P("rank", "dp"),
        P("rank", "dp"),
        P("rank"),
    )
    out_specs = (P("rank", "dp"), P("rank", "dp"), P("rank"))
    if mesh.shape["rank"] == 1 and mesh.shape["dp"] % PLANE == 0:
        body = fused
    else:
        body = shards
    return jax.shard_map(body, mesh=mesh, in_specs=in_specs, out_specs=out_specs, check_vma=False)
```

```python
import functools
import math

import jax
import jax.numpy as jnp
from jax import lax
from jax.experimental import pallas as pl
from jax.experimental.pallas import tpu as pltpu
from jax.sharding import PartitionSpec as P

RANK = 256
INNER = 4
MIRROR = 3


exact_mode = lax.Precision.HIGHEST
step_size = 2.0


def moments(cloud, factor):
    product = jnp.dot(cloud, factor.T, precision=exact_mode)
    square = jnp.dot(factor, jnp.sum(cloud * cloud, axis=0), precision=exact_mode)
    column = jnp.sum(factor, axis=1)
    return (product, square, column)


def widen(local_part, offset):
    shape_full = local_part.shape[:-1] + (RANK,)
    starts = (0,) * (local_part.ndim - 1) + (offset,)
    return lax.dynamic_update_slice(jnp.zeros(shape_full, jnp.float32), local_part, starts)


def narrow(full_part, offset, ranks_local):
    return lax.dynamic_slice_in_dim(full_part, offset, ranks_local, full_part.ndim - 1)


def shards(cloud_x, cloud_y, mass_x, mass_y, left_start, right_start, weight_start):
    ranks_local = left_start.shape[0]
    points_dev = left_start.shape[1]
    total_count = float(points_dev * lax.axis_size("dp"))
    offset = lax.axis_index("rank") * ranks_local
    mass_sums = lax.psum((jnp.sum(mass_x), jnp.sum(mass_y)), "dp")
    left_mass = mass_x * (total_count / mass_sums[0])
    right_mass = mass_y * (total_count / mass_sums[1])

    def project(kernel_left, kernel_right, kernel_weight):
        scale_left = jnp.ones((ranks_local,), jnp.float32)
        scale_right = jnp.ones((ranks_local,), jnp.float32)
        for repeat in range(INNER):
            row_left, row_right = lax.psum(
                (
                    jnp.dot(scale_left, kernel_left, precision=exact_mode),
                    jnp.dot(scale_right, kernel_right, precision=exact_mode),
                ),
                "rank",
            )
            point_left = left_mass / row_left
            point_right = right_mass / row_right
            column_left, column_right = lax.psum(
                (
                    jnp.dot(kernel_left, point_left, precision=exact_mode),
                    jnp.dot(kernel_right, point_right, precision=exact_mode),
                ),
                "dp",
            )
            weights = jnp.cbrt(
                kernel_weight * scale_left * column_left * scale_right * column_right
            )
            scale_left = weights / column_left
            scale_right = weights / column_right
        left = point_left[None, :] * kernel_left * scale_left[:, None]
        right = point_right[None, :] * kernel_right * scale_right[:, None]
        return (left, right, weights)

    left, right, weights = project(left_start, right_start, weight_start)
    for outer in range(MIRROR):
        prod_x, square_x, sums_q = moments(cloud_x, left)
        prod_y, square_y, sums_r = moments(cloud_y, right)
        root_weights = jnp.where(lax.axis_index("dp") == 0, weights, jnp.zeros_like(weights))
        full_px, full_py, full_sx, full_sy, full_q, full_r, full_w = lax.psum(
            (
                widen(prod_x, offset),
                widen(prod_y, offset),
                widen(square_x, offset),
                widen(square_y, offset),
                widen(sums_q, offset),
                widen(sums_r, offset),
                widen(root_weights, offset),
            ),
            ("dp", "rank"),
        )
        full_gq = full_sy / full_w
        full_gr = full_sx / full_w
        full_gg = -(
            full_sx * full_r + full_q * full_sy - 2.0 * jnp.sum(full_px * full_py, axis=0)
        ) / (full_w * full_w)
        mean_q = jnp.sum(full_gq) / RANK
        mean_r = jnp.sum(full_gr) / RANK
        mean_g = jnp.sum(full_gg) / RANK
        prod_x = narrow(full_px, offset, ranks_local)
        prod_y = narrow(full_py, offset, ranks_local)
        grad_q = narrow(full_gq, offset, ranks_local)
        grad_r = narrow(full_gr, offset, ranks_local)
        grad_g = narrow(full_gg, offset, ranks_local)
        field_q = (grad_q - mean_q)[:, None] - 2.0 * jnp.dot(
            prod_y.T, cloud_x, precision=exact_mode
        ) / weights[:, None]
        field_r = (grad_r - mean_r)[:, None] - 2.0 * jnp.dot(
            prod_x.T, cloud_y, precision=exact_mode
        ) / weights[:, None]
        kernel_left = left * jnp.exp(-step_size * field_q)
        kernel_right = right * jnp.exp(-step_size * field_r)
        kernel_weight = weights * jnp.exp(-step_size * (grad_g - mean_g))
        left, right, weights = project(kernel_left, kernel_right, kernel_weight)
    return (RANK * left, RANK * right, weights * (RANK / total_count))


PLANE = 8
LANE = 128
AUG = 80
LOG2E = math.log2(math.e)
MESH = pl.DeviceIdType.MESH


def split(x):
    high = x.astype(jnp.bfloat16)
    low = (x - high.astype(jnp.float32)).astype(jnp.bfloat16)
    return high, low


def cube_root(x):
    y = jnp.exp(jnp.log(x) * (1.0 / 3.0))
    y = y - (y - x / (y * y)) * (1.0 / 3.0)
    return jnp.where(x > 0.0, y, x)


def fused_kernel(
    devices,
    cx_ref, cy_ref, mx_ref, my_ref, ls_ref, rs_ref, ws_ref,
    kl, kr, wo_ref,
    vl, vr, ul, ur, pl_ref, pr_ref,
    xh, xl, yh, yl, mom, weight_ref, sl_ref, sr_ref, coef_h, coef_l,
    pay, got1, bpay, bgot1,
    cgot1, cpay2, cgot2, full,
    s_sem1, r_sem1, s_sem3, r_sem3, bs_sem1, br_sem1,
    cs_sem1, cr_sem1, cs_sem2, cr_sem2, in_sem,
):
    ranks, points = ls_ref.shape
    dims = cx_ref.shape[0]
    total_count = float(points * devices)
    planes = devices // PLANE
    halves = ranks // LANE
    tiles = points // LANE
    blocks = ranks // 8
    me = lax.axis_index("dp")
    spot = lax.rem(me, PLANE)
    level = lax.div(me, PLANE)

    def in_plane(shift):
        return level * PLANE + lax.rem(spot + shift, PLANE)

    def across(shift):
        return lax.rem(level + shift, planes) * PLANE + spot

    loads = [
        pltpu.make_async_copy(src, dst, in_sem.at[i])
        for i, (src, dst) in enumerate(((ls_ref, kl), (rs_ref, kr)))
    ]
    for load in loads:
        load.start()
    barrier = pltpu.get_barrier_semaphore()
    for shift in range(1, devices):
        pl.semaphore_signal(barrier, inc=1, device_id={"dp": lax.rem(me + shift, devices)}, device_id_type=MESH)

    def send(src, dst, s_sem, r_sem, target):
        copy = pltpu.make_async_remote_copy(
            src_ref=src, dst_ref=dst, send_sem=s_sem, recv_sem=r_sem,
            device_id={"dp": target}, device_id_type=MESH,
        )
        copy.start()
        return copy

    def scatter_across(src, got, s_sems, r_sems):
        return [
            send(src, got.at[level], s_sems.at[shift], r_sems.at[shift], across(shift))
            for shift in range(1, planes)
        ]

    def finish(copies):
        for copy in copies:
            copy.wait_recv()
        for copy in copies:
            copy.wait_send()

    def total_of(got, count):
        acc = got[0]
        for i in range(1, count):
            acc = acc + got[i]
        return acc

    def exchange_all(src, got, s_sems, r_sems):
        copies = []
        for climb in range(planes):
            for shift in range(PLANE):
                step = climb * PLANE + shift
                if step == 0:
                    continue
                target = lax.rem(level + climb, planes) * PLANE + lax.rem(spot + shift, PLANE)
                copies.append(send(src, got.at[me], s_sems.at[step], r_sems.at[step], target))
        return copies

    def tree(got):
        parts = [got[i] for i in range(devices)]
        while len(parts) > 1:
            pairs = [parts[i] + parts[i + 1] for i in range(0, len(parts) - 1, 2)]
            parts = pairs + ([parts[-1]] if len(parts) % 2 else [])
        return parts[0]

    def small_reduce(value, parity):
        src, got = pay.at[parity], got1.at[parity]
        src[...] = value
        got[me] = value
        finish(exchange_all(src, got, s_sem1.at[parity], r_sem1.at[parity]))
        return tree(got)

    def spread(dst, value):
        for h in range(halves):
            square = jnp.broadcast_to(value[h : h + 1, :], (LANE, LANE))
            dst[h * LANE : (h + 1) * LANE, :] = square.T

    def row_of(b):
        return pl.ds(pl.multiple_of(b * 8, 8), 8)

    def rows_pass():
        def body(b, acc):
            al, ar = acc
            rows = row_of(b)
            al = al + kl[rows, :] * jnp.concatenate([vl[rows, :]] * tiles, axis=1)
            ar = ar + kr[rows, :] * jnp.concatenate([vr[rows, :]] * tiles, axis=1)
            return al, ar

        zero = jnp.zeros((8, points), jnp.float32)
        al, ar = lax.fori_loop(0, blocks, body, (zero, zero), unroll=4)
        ul[...] = jnp.broadcast_to(sl_ref[...] / jnp.sum(al, axis=0, keepdims=True), (8, points))
        ur[...] = jnp.broadcast_to(sr_ref[...] / jnp.sum(ar, axis=0, keepdims=True), (8, points))

    def columns_pass():
        bl, br = ul[...], ur[...]

        def fold(x):
            parts = [x[:, i * LANE : (i + 1) * LANE] for i in range(tiles)]
            while len(parts) > 1:
                parts = [parts[i] + parts[i + 1] for i in range(0, len(parts) - 1, 2)] + (
                    parts[-1:] if len(parts) % 2 else []
                )
            return parts[0]

        def body(b, carry):
            rows = row_of(b)
            pl_ref[rows, :] = fold(kl[rows, :] * bl)
            pr_ref[rows, :] = fold(kr[rows, :] * br)
            return carry

        lax.fori_loop(0, blocks, body, 0, unroll=4)
        out = []
        for ref in (pl_ref, pr_ref):
            for h in range(halves):
                out.append(jnp.sum(ref[h * LANE : (h + 1) * LANE, :].T, axis=0, keepdims=True))
        return jnp.concatenate(out, axis=0)

    def rescale(cl, cr, v1, v2):
        g = cube_root(weight_ref[...] * v1 * cl * v2 * cr)
        v1, v2 = g / cl, g / cr
        spread(vl, v1)
        spread(vr, v2)
        return g, v1, v2

    def small_step(parity, v1, v2):
        rows_pass()
        sums = small_reduce(columns_pass(), parity)
        return rescale(sums[:halves], sums[halves : 2 * halves], v1, v2)

    for src, high, low in ((cx_ref, xh, xl), (cy_ref, yh, yl)):
        cloud = src[...]
        square = jnp.sum(cloud * cloud, axis=0, keepdims=True)
        place = lax.broadcasted_iota(jnp.int32, (LANE - dims, points), 0)
        extra = jnp.where(place == 0, square, jnp.where(place == 1, 1.0, 0.0))
        high[:dims, :], low[:dims, :] = split(cloud)
        high[dims:, :], low[dims:, :] = split(extra)
    ones = jnp.ones((halves, LANE), jnp.float32)
    weight_ref[...] = ws_ref[...]
    vl[...] = jnp.ones((ranks, LANE), jnp.float32)
    vr[...] = jnp.ones((ranks, LANE), jnp.float32)
    sl_ref[...] = mx_ref[...]
    sr_ref[...] = my_ref[...]
    for load in loads:
        load.wait()
    rows_pass()
    first = columns_pass()
    pl.semaphore_wait(barrier, devices - 1)

    sums = small_reduce(first, 0)
    cl, cr = sums[:halves], sums[halves : 2 * halves]
    al = total_count / jnp.sum(cl)
    ar = total_count / jnp.sum(cr)
    sl_ref[...] = sl_ref[...] * al
    sr_ref[...] = sr_ref[...] * ar
    g, v1, v2 = rescale(cl * al, cr * ar, ones, ones)

    def inner(i, carry):
        _, v1, v2 = carry
        return small_step(lax.rem(i, 2), v1, v2)

    _, v1, v2 = lax.fori_loop(1, INNER - 1, inner, (g, v1, v2))

    chunk = 2 * LANE

    def moment_pass(k_ref, u_ref, high, low):
        acc = jnp.zeros((AUG, ranks), jnp.float32)
        nt = (((1,), (1,)), ((), ()))
        for c in range(points // chunk):
            cols = slice(c * chunk, (c + 1) * chunk)
            w = k_ref[:, cols] * u_ref[0:1, cols]
            wh, wl = split(w)
            h, l = high[:AUG, cols], low[:AUG, cols]
            acc = acc + lax.dot_general(h, wh, nt, preferred_element_type=jnp.float32)
            acc = acc + lax.dot_general(h, wl, nt, preferred_element_type=jnp.float32)
            acc = acc + lax.dot_general(l, wh, nt, preferred_element_type=jnp.float32)
        return acc

    def lanes(row):
        return [row[:, h * LANE : (h + 1) * LANE] for h in range(halves)]

    def wide(value):
        return jnp.concatenate([value[h : h + 1, :] for h in range(halves)], axis=1)

    def update(k_ref, u_ref, v_ref, high, low):
        for c in range(points // chunk):
            cols = slice(c * chunk, (c + 1) * chunk)
            h, l = high[:, cols], low[:, cols]
            a, b = coef_h[...], coef_l[...]
            e = jnp.dot(a, h, preferred_element_type=jnp.float32)
            e = e + jnp.dot(a, l, preferred_element_type=jnp.float32)
            e = e + jnp.dot(b, h, preferred_element_type=jnp.float32)
            scale = jnp.concatenate([v_ref[...]] * (chunk // LANE), axis=1)
            k_ref[:, cols] = k_ref[:, cols] * u_ref[0:1, cols] * scale * jnp.exp2(e)

    per = dims // PLANE

    def coefficients(centre, moment):
        mean = jnp.sum(moment) / ranks
        bias = (-2.0 * LOG2E) * (moment - mean)
        place = lax.broadcasted_iota(jnp.int32, (LANE - dims, ranks), 0)
        extra = jnp.where(place == 1, bias, 0.0)
        full_rows = jnp.concatenate([centre * (4.0 * LOG2E), extra], axis=0)
        high, low = split(full_rows.T)
        coef_h[...] = high
        coef_l[...] = low

    def outer_step(outer, carry):
        v1, v2 = carry
        rows_pass()
        mom_x = moment_pass(kl, ul, xh, xl)
        mom_y = moment_pass(kr, ur, yh, yl)
        for j in range(PLANE):
            mom[j, 0] = mom_x[j * per : (j + 1) * per]
            mom[j, 1] = mom_y[j * per : (j + 1) * per]
        copies = []
        for shift in range(1, PLANE):
            target = lax.rem(spot + shift, PLANE)
            copies.append(
                send(mom.at[target], cgot1.at[spot], cs_sem1.at[shift], cr_sem1.at[shift], in_plane(shift))
            )
        cgot1[spot] = mom[spot]
        value = jnp.concatenate(
            lanes(mom_x[dims + 1 : dims + 2]) + lanes(mom_y[dims + 1 : dims + 2])
            + lanes(mom_x[dims : dims + 1]) + lanes(mom_y[dims : dims + 1]),
            axis=0,
        )
        bpay[...] = value
        bgot1[me] = value
        small = exchange_all(bpay, bgot1, bs_sem1, br_sem1)
        finish(copies)
        part = total_of(cgot1, PLANE)
        cpay2[...] = part
        cgot2[level] = part
        copies = scatter_across(cpay2, cgot2, cs_sem2, cr_sem2)
        finish(small)
        sums = tree(bgot1)
        cl, cr = sums[:halves], sums[halves : 2 * halves]
        sx = wide(sums[2 * halves : 3 * halves] / cl)
        sy = wide(sums[3 * halves : 4 * halves] / cr)
        g, v1, v2 = rescale(cl, cr, v1, v2)
        finish(copies)
        full[spot] = total_of(cgot2, planes)
        finish(
            [
                send(full.at[spot], full.at[spot], s_sem3.at[shift], r_sem3.at[shift], in_plane(shift))
                for shift in range(1, PLANE)
            ]
        )
        inv_l, inv_r = wide(1.0 / cl), wide(1.0 / cr)
        centre_x = jnp.concatenate([full[j, 0] for j in range(PLANE)], axis=0) * inv_l
        centre_y = jnp.concatenate([full[j, 1] for j in range(PLANE)], axis=0) * inv_r
        coefficients(centre_y, sy)
        update(kl, ul, vl, xh, xl)
        coefficients(centre_x, sx)
        update(kr, ur, vr, yh, yl)
        gg = -(sx + sy - 2.0 * jnp.sum(centre_x * centre_y, axis=0, keepdims=True))
        tilt = jnp.exp(-step_size * (gg - jnp.sum(gg) / ranks))
        weight_ref[...] = g * jnp.concatenate(lanes(tilt), axis=0)
        vl[...] = jnp.ones((ranks, LANE), jnp.float32)
        vr[...] = jnp.ones((ranks, LANE), jnp.float32)
        carry = (g, ones, ones)
        steps = jnp.where(outer == MIRROR - 1, INNER, INNER - 1)

        def again(i, carry):
            return small_step(lax.rem(i + 1, 2), carry[1], carry[2])

        g, v1, v2 = lax.fori_loop(0, steps, again, carry)
        wo_ref[...] = g * (ranks / total_count)
        return v1, v2

    lax.fori_loop(0, MIRROR, outer_step, (v1, v2))

    def emit(b, carry):
        rows = row_of(b)
        sl = jnp.concatenate([vl[rows, :]] * tiles, axis=1)
        sr = jnp.concatenate([vr[rows, :]] * tiles, axis=1)
        kl[rows, :] = kl[rows, :] * ul[...] * sl * float(ranks)
        kr[rows, :] = kr[rows, :] * ur[...] * sr * float(ranks)
        return carry

    lax.fori_loop(0, blocks, emit, 0)


def fused(cloud_x, cloud_y, mass_x, mass_y, left_start, right_start, weight_start):
    devices = lax.axis_size("dp")
    ranks, points = left_start.shape
    dims = cloud_x.shape[0]
    planes = devices // PLANE
    halves = ranks // LANE
    per = dims // PLANE
    f32 = jnp.float32
    dma = pltpu.SemaphoreType.DMA
    vmem = pl.BlockSpec(memory_space=pltpu.VMEM)
    left, right, weights = pl.pallas_call(
        functools.partial(fused_kernel, devices),
        out_shape=(
            jax.ShapeDtypeStruct((ranks, points), f32),
            jax.ShapeDtypeStruct((ranks, points), f32),
            jax.ShapeDtypeStruct((halves, LANE), f32),
        ),
        in_specs=[vmem] * 4 + [pl.BlockSpec(memory_space=pl.ANY)] * 2 + [vmem],
        out_specs=(vmem,) * 3,
        scratch_shapes=[
            pltpu.VMEM((ranks, LANE), f32),
            pltpu.VMEM((ranks, LANE), f32),
            pltpu.VMEM((8, points), f32),
            pltpu.VMEM((8, points), f32),
            pltpu.VMEM((ranks, LANE), f32),
            pltpu.VMEM((ranks, LANE), f32),
            pltpu.VMEM((LANE, points), jnp.bfloat16),
            pltpu.VMEM((LANE, points), jnp.bfloat16),
            pltpu.VMEM((LANE, points), jnp.bfloat16),
            pltpu.VMEM((LANE, points), jnp.bfloat16),
            pltpu.VMEM((PLANE, 2, per, ranks), f32),
            pltpu.VMEM((halves, LANE), f32),
            pltpu.VMEM((1, points), f32),
            pltpu.VMEM((1, points), f32),
            pltpu.VMEM((ranks, LANE), jnp.bfloat16),
            pltpu.VMEM((ranks, LANE), jnp.bfloat16),
            pltpu.VMEM((2, 2 * halves, LANE), f32),
            pltpu.VMEM((2, devices, 2 * halves, LANE), f32),
            pltpu.VMEM((4 * halves, LANE), f32),
            pltpu.VMEM((devices, 4 * halves, LANE), f32),
            pltpu.VMEM((PLANE, 2, per, ranks), f32),
            pltpu.VMEM((2, per, ranks), f32),
            pltpu.VMEM((planes, 2, per, ranks), f32),
            pltpu.VMEM((PLANE, 2, per, ranks), f32),
            dma((2, devices)), dma((2, devices)), dma((PLANE,)), dma((PLANE,)), dma((devices,)), dma((devices,)),
            dma((PLANE,)), dma((PLANE,)), dma((planes,)), dma((planes,)), dma((2,)),
        ],
        compiler_params=pltpu.CompilerParams(
            collective_id=0, has_side_effects=True, vmem_limit_bytes=63 * 1024 * 1024
        ),
        name="sinkhorn",
    )(
        cloud_x, cloud_y, mass_x.reshape(1, points), mass_y.reshape(1, points),
        left_start, right_start, weight_start.reshape(halves, LANE),
    )
    return left, right, weights.reshape(ranks)


def solution(mesh):
    in_specs = (
        P(None, "dp"),
        P(None, "dp"),
        P("dp"),
        P("dp"),
        P("rank", "dp"),
        P("rank", "dp"),
        P("rank"),
    )
    out_specs = (P("rank", "dp"), P("rank", "dp"), P("rank"))
    if mesh.shape["rank"] == 1 and mesh.shape["dp"] % PLANE == 0:
        body = fused
    else:
        body = shards
    return jax.shard_map(body, mesh=mesh, in_specs=in_specs, out_specs=out_specs, check_vma=False)
```
